32 devices in a mesh: member: 2 (over x), lat: 16 (over z, y, core).
Axes of the slice: x: 2, y: 2, z: 4, core: 2. Of those that a mesh axis runs over, the one named last changes fastest.
Arguments:
- height: float32 [128, 32, 1440], P(('member', 'lat')), parts along dimension 0, may hold values from -6 to 6
- zonal_courant: float32 [128, 32, 1440], P(('member', 'lat')), parts along dimension 0, may hold values from -1.5 to 1.5
- merid_courant: float32 [128, 32, 1440], P(('member', 'lat')), parts along dimension 0, may hold values from -1.5 to 1.5
- rates: float32 [64], P('member'), parts along dimension 0, may hold values from 0.05 to 0.5
- thresholds: float32 [64], P('member'), parts along dimension 0, may hold values from -3 to 3
- flags: int32 [64], replicated, may hold values from 0 to 1, as said below
- cutoffs: int32 [64], replicated, may hold values from 45 to 360
Outputs:
- filtered_height: float32 [128, 32, 1440], P(('member', 'lat')), parts along dimension 0
The draws below stay inside these ranges and needn't reach their ends.
There are 2 independent parts, one for each index of `member`. The reference program is written for one: setup_inputs(seed, part) draws one part's arguments, and reference() takes and returns one part's arrays. A program takes and returns all parts, laid end to end along the dimension named above; an argument that names none is the same for every part. Nothing has to cross between parts.
Inputs may be any that keep to these rules, and one draw needn't show every extreme that they name: flags is 1 on a southern band of rows that starts at row 0 and on a northern band that ends at row 63, each band 64 // 8 to 16 rows long, and 0 on all other rows.
All inputs are finite; a program needn't handle non-finite values.
Results may differ from the reference program's by a relative error of at most 0.00007.
Values sent between devices are 32-bit elements; how exact they have to be, the bound alone decides.
A program may use at most 64 MiB of HBM per device.

```python
import math
import jax
import jax.numpy as jnp

NLON = 1440
LEV = 32
NLAT = 64


def draw_flags(key, part):
    south_key = jax.random.fold_in(key, 11)
    north_key = jax.random.fold_in(key, 23)
    south = jax.random.randint(south_key, (), NLAT // 8, NLAT // 4 + 1)
    north = jax.random.randint(north_key, (), NLAT // 8, NLAT // 4 + 1)
    rows = jnp.arange(NLAT, dtype=jnp.int32)
    return ((rows < south) | (rows >= NLAT - north)).astype(jnp.int32)


def with_ends(drawn, stream_key, low, high):
    spot = [jax.random.randint(jax.random.fold_in(stream_key, axis), (), 0, length) for axis, length in enumerate(drawn.shape)]
    widest = drawn.shape.index(max(drawn.shape))
    beside = spot[:widest] + [(spot[widest] + 1) % drawn.shape[widest]] + spot[widest + 1:]
    return drawn.at[tuple(spot)].set(low).at[tuple(beside)].set(high)


def block_levels(rng, shape, cuts, smallest, high):
    loudness = 1.0
    for axis_at, blocks in cuts:
        draws = jax.random.uniform(jax.random.fold_in(jax.random.fold_in(rng, 6), axis_at), (blocks,), jnp.float32, smallest / len(cuts), high / len(cuts))
        loudness = loudness * jnp.repeat(jnp.exp(draws), shape[axis_at] // blocks).reshape((-1,) + (1,) * (len(shape) - 1 - axis_at))
    return loudness


def normal_values(own_key, shape, scale, bound, pieces=(), kind=jnp.bfloat16):
    gain = block_levels(own_key, shape, pieces, -0.22, 0.18) if pieces else 1.0
    result = jax.random.normal(own_key, shape, jnp.float32) * scale * gain
    return jnp.minimum(jnp.maximum(result, -bound), bound).astype(kind)


def setup_inputs(seed: int = 0, part: int = 0) -> dict:
    splits = jax.random.split(jax.random.key(seed), 8)
    part_splits = jax.random.split(jax.random.fold_in(splits[7], part), 8)
    return {
        "height": normal_values(part_splits[0], (NLAT, LEV, NLON), 1.0, 6.0, ((0, 16),), jnp.float32),
        "zonal_courant": normal_values(part_splits[1], (NLAT, LEV, NLON), 0.3, 1.5, ((0, 16),), jnp.float32),
        "merid_courant": normal_values(part_splits[2], (NLAT, LEV, NLON), 0.3, 1.5, ((0, 16),), jnp.float32),
        "rates": jnp.clip(jnp.exp(jax.random.uniform(part_splits[3], (LEV,), jnp.float32, math.log(0.05), math.log(0.5))), 0.05, 0.5),
        "thresholds": normal_values(part_splits[4], (LEV,), 1.0, 3.0, (), jnp.float32),
        "flags": draw_flags(jax.random.fold_in(splits[7], 71), part),
        "cutoffs": with_ends(jax.random.randint(splits[6], (NLAT,), NLON // 32, NLON // 4 + 1), jax.random.fold_in(splits[6], 1), NLON // 32, (NLON // 4 + 1) - 1).astype(jnp.int32),
    }


def reference(height, zonal_courant, merid_courant, rates, thresholds, flags, cutoffs):
    rows = jnp.arange(NLAT, dtype=jnp.int32)
    cos_rows = jnp.sin(jnp.pi * (rows.astype(jnp.float32) + 0.5) / NLAT)
    faces = jnp.arange(NLAT + 1, dtype=jnp.int32)
    cos_faces = jnp.where((faces > 0) & (faces < NLAT), jnp.sin(jnp.pi * faces.astype(jnp.float32) / NLAT), jnp.float32(0.0))
    east = jnp.roll(height, -1, axis=2)
    west = jnp.roll(height, 1, axis=2)
    far_east = jnp.roll(height, -2, axis=2)
    face_height = (7.0 * (height + east) - (west + far_east)) / 12.0
    face_speed = 0.5 * (zonal_courant + jnp.roll(zonal_courant, -1, axis=2))
    zonal_flux = face_speed * face_height
    zonal_div = zonal_flux - jnp.roll(zonal_flux, 1, axis=2)
    padded_height = jnp.pad(height, ((2, 2), (0, 0), (0, 0)))
    padded_speed = jnp.pad(merid_courant, ((2, 2), (0, 0), (0, 0)))
    count = NLAT + 1
    merid_face = (7.0 * (padded_height[1:count + 1] + padded_height[2:count + 2]) - (padded_height[0:count] + padded_height[3:count + 3])) / 12.0
    merid_speed = 0.5 * (padded_speed[1:count + 1] + padded_speed[2:count + 2]) * cos_faces[:, None, None]
    merid_flux = merid_speed * merid_face
    merid_div = (merid_flux[1:] - merid_flux[:-1]) / cos_rows[:, None, None]
    source = -rates[None, :, None] * jax.nn.softplus(height - thresholds[None, :, None])
    level_mean = jnp.sum(jnp.sum(source, axis=2) * cos_rows[:, None], axis=0) / (NLON * jnp.sum(cos_rows))
    updated = height - zonal_div - merid_div + source - level_mean[None, :, None]
    waves = jnp.maximum(jnp.arange(NLON // 2 + 1), 1).astype(jnp.float32)
    ratio = cutoffs.astype(jnp.float32)[:, None] / waves[None, :]
    damp = jnp.where(flags[:, None] > 0, jnp.minimum(1.0, ratio * ratio), 1.0)
    spectrum = jnp.fft.rfft(updated, axis=2)
    filtered = jnp.fft.irfft(spectrum * damp[:, None, :], n=NLON, axis=2)
    return filtered.astype(jnp.float32)
```

```python
import functools

import jax
import jax.numpy as jnp
import numpy as np
from jax import lax
from jax.experimental import pallas as pl
from jax.experimental.pallas import tpu as pltpu
from jax.sharding import PartitionSpec as P

CHUNKS = 2
GROUP = 8
BF = jnp.bfloat16
F32 = jnp.float32


def split_table(table):
    high = table.astype(jnp.bfloat16)
    low = (table - high.astype(np.float64)).astype(jnp.bfloat16)
    return np.stack([high, low])


def cas(angle):
    return np.cos(angle) + np.sin(angle)


def filter_tables(nlon):
    quarter, half = nlon // 4, nlon // 2
    m = np.arange(quarter)
    zero = cas(2 * np.pi * (np.outer(m, m) % quarter) / quarter)
    odd = 2 * np.arange(half) + 1
    two = cas(2 * np.pi * (np.outer(odd[:quarter], odd[:quarter]) % nlon) / nlon)
    ones = cas(np.pi * (np.outer(odd, odd) % (2 * nlon)) / nlon)
    return split_table(np.stack([zero, two], 0)), split_table(ones)


def latitude_table(nlat):
    rows = np.sin(np.pi * (np.arange(nlat) + 0.5) / nlat)
    faces = np.sin(np.pi * np.arange(nlat + 1) / nlat)
    faces[0] = faces[-1] = 0.0
    table = np.zeros((3, nlat + 1), np.float32)
    table[0] = faces / 24.0
    table[1, :nlat] = rows
    table[2, :nlat] = 1.0 / rows
    return table, float(np.sum(rows))


def shifted(x, s):
    return jnp.concatenate([x[:, s:], x[:, :s]], axis=1)


def halves(x):
    high = x.astype(BF)
    return high, (x - high.astype(F32)).astype(BF)


def product(x, high_table, low_table):
    high, low = halves(x)
    rows = x.shape[0]
    both = jnp.dot(
        jnp.concatenate([high, low], axis=0), high_table, preferred_element_type=F32
    )
    return both[:rows] + both[rows:] + jnp.dot(high, low_table, preferred_element_type=F32)


def kernel(
    n, area,
    lat_ref, flags_ref, cutoffs_ref, rates_ref, thresholds_ref,
    h_hbm, z_hbm, m_hbm, quarter_hbm, half_hbm,
    out_hbm,
    h, z, m, quarter_t, half_t, base, result, sides, part, mine, others,
    hl, ml, hr, mr,
    in_sem, out_sem, halo_send, halo_recv, sum_send, sum_recv,
):
    rows, levels, nlon = h.shape
    me = lax.axis_index("lat")
    first = me * rows
    groups = levels // GROUP
    width = levels // CHUNKS

    loads = [
        pltpu.make_async_copy(src, dst, in_sem.at[i])
        for i, (src, dst) in enumerate(
            [(h_hbm, h), (z_hbm, z), (m_hbm, m), (quarter_hbm, quarter_t), (half_hbm, half_t)]
        )
    ]
    for load in loads:
        load.start()

    barrier = pltpu.get_barrier_semaphore()

    def greet(o, c):
        pl.semaphore_signal(barrier, inc=1, device_id={"lat": lax.rem(me + o, n)})
        return c

    lax.fori_loop(1, n, greet, 0)
    pl.semaphore_wait(barrier, n - 1)

    def halo_copies(c, side):
        at = pl.ds(c * width, width)
        if side == 0:
            pairs = [
                (h_hbm.at[pl.ds(rows - 2, 2), at], hl.at[:, at]),
                (m_hbm.at[rows - 1, at], ml.at[at]),
            ]
            target = me + 1
        else:
            pairs = [
                (h_hbm.at[pl.ds(0, 2), at], hr.at[:, at]),
                (m_hbm.at[0, at], mr.at[at]),
            ]
            target = me - 1
        return [
            pltpu.make_async_remote_copy(
                src, dst, halo_send.at[side, c, i], halo_recv.at[side, c, i],
                device_id={"lat": target},
            )
            for i, (src, dst) in enumerate(pairs)
        ]

    def start_halo(side):
        for c in range(CHUNKS):
            for copy in halo_copies(c, side):
                copy.start()

    pl.when(me < n - 1)(lambda: start_halo(0))
    pl.when(me > 0)(lambda: start_halo(1))

    @pl.when(me == 0)
    def _():
        hl[...] = jnp.zeros_like(hl)
        ml[...] = jnp.zeros_like(ml)

    @pl.when(me == n - 1)
    def _():
        hr[...] = jnp.zeros_like(hr)
        mr[...] = jnp.zeros_like(mr)

    lane = lax.broadcasted_iota(jnp.int32, (levels, levels), 1)
    diagonal = lane == lax.broadcasted_iota(jnp.int32, (levels, levels), 0)

    def column(row):
        spread = jnp.where(diagonal, jnp.broadcast_to(row, (levels, levels)), 0.0)
        return jnp.sum(spread, axis=1, keepdims=True)

    sides[0] = jnp.broadcast_to(column(rates_ref[...]), (levels, 128))
    sides[1] = jnp.broadcast_to(column(thresholds_ref[...]), (levels, 128))

    loads[0].wait()
    loads[1].wait()

    def local_terms(g, carry):
        at = pl.ds(pl.multiple_of(g * GROUP, GROUP), GROUP)
        rate = sides[0, at, :][:, :1]
        threshold = sides[1, at, :][:, :1]
        weighted = jnp.zeros((GROUP, nlon), F32)
        for r in range(rows):
            hh = h[r, at, :]
            zz = z[r, at, :]
            face = 7.0 * (hh + shifted(hh, 1)) - (shifted(hh, nlon - 1) + shifted(hh, 2))
            flux = (zz + shifted(zz, 1)) * face * (1.0 / 24.0)
            source = -rate * jnp.log(1.0 + jnp.exp(hh - threshold))
            base[r, at, :] = hh - (flux - shifted(flux, nlon - 1)) + source
            weighted = weighted + source * lat_ref[1, first + r]
        total = jnp.sum(weighted, axis=1, keepdims=True)
        part[at, :] = jnp.broadcast_to(total, (GROUP, 128))
        return carry

    lax.fori_loop(0, groups, local_terms, 0)

    wide = lax.broadcasted_iota(jnp.int32, (levels, 128), 1)
    tall = lax.broadcasted_iota(jnp.int32, (levels, 128), 0)
    mine[...] = jnp.sum(jnp.where(wide == tall, part[...], 0.0), axis=0, keepdims=True)

    def sum_copy(o):
        return pltpu.make_async_remote_copy(
            mine, others.at[o - 1], sum_send.at[o - 1], sum_recv.at[o - 1],
            device_id={"lat": lax.rem(me + o, n)},
        )

    def send_sum(o, c):
        sum_copy(o).start()
        return c

    lax.fori_loop(1, n, send_sum, 0)

    quarter, half = nlon // 4, nlon // 2

    def factors(length, step, offset):
        k = lax.broadcasted_iota(jnp.int32, (1, length), 1) * step + offset
        k = jnp.maximum(jnp.minimum(k, nlon - k), 1).astype(F32)
        out = []
        for r in range(rows):
            ratio = cutoffs_ref[first + r].astype(F32) / k
            factor = (1.0 - jnp.minimum(1.0, ratio * ratio)) * (1.0 / nlon)
            on = jnp.where(flags_ref[first + r] > 0, 1.0, 0.0)
            out.append(factor * on)
        return out

    all_factors = [factors(quarter, 4, 0), factors(quarter, 4, 2), factors(half, 2, 1)]

    def removed(x, high_table, low_table, factor):
        spectrum = product(x, high_table, low_table).reshape(rows, width, x.shape[1])
        scaled = jnp.concatenate([spectrum[r] * factor[r] for r in range(rows)], axis=0)
        return product(scaled, high_table, low_table)

    loads[2].wait()

    def merid(c):
        def body(g, carry):
            at = pl.ds(pl.multiple_of(c * width + g * GROUP, GROUP), GROUP)

            def height(i):
                return hl[i + 2, at, :] if i < 0 else hr[i - rows, at, :] if i >= rows else h[i, at, :]

            def speed(i):
                return ml[at, :] if i < 0 else mr[at, :] if i >= rows else m[i, at, :]

            previous = None
            for f in range(rows + 1):
                face = 7.0 * (height(f - 1) + height(f)) - (height(f - 2) + height(f + 1))
                flux = (speed(f - 1) + speed(f)) * face * lat_ref[0, first + f]
                if f > 0:
                    base[f - 1, at, :] -= (flux - previous) * lat_ref[2, first + f - 1]
                previous = flux
            return carry

        lax.fori_loop(0, width // GROUP, body, 0)

    mean = None
    stores = []
    for c in range(CHUNKS):
        @pl.when(me > 0)
        def _():
            for copy in halo_copies(c, 0):
                copy.wait_recv()

        @pl.when(me < n - 1)
        def _():
            for copy in halo_copies(c, 1):
                copy.wait_recv()

        merid(c)
        if c == 0:
            loads[3].wait()
            loads[4].wait()
        at = pl.ds(c * width, width)
        x = base[:, at, :].reshape(rows * width, nlon)
        near, far = x[:, :half], x[:, half:]
        even, odd = near + far, near - far
        left, right = even[:, :quarter], even[:, quarter:]
        zero = removed(left + right, quarter_t[0, 0], quarter_t[1, 0], all_factors[0])
        two = removed(left - right, quarter_t[0, 1], quarter_t[1, 1], all_factors[1])
        ones = removed(odd, half_t[0], half_t[1], all_factors[2])
        even = jnp.concatenate([zero + two, zero - two], axis=1)
        if c == 0:
            def wait_sum(o, carry):
                sum_copy(o).wait()
                return carry

            lax.fori_loop(1, n, wait_sum, 0)
            total = mine[...] + jnp.sum(others[...], axis=0)
            mean = column(total[:, :levels]) * (1.0 / area)
        kept = jnp.concatenate([near - even - ones, far - even + ones], axis=1)
        kept = kept.reshape(rows, width, nlon) - mean[c * width : (c + 1) * width][None]
        result[:, at, :] = kept
        store = pltpu.make_async_copy(result.at[:, at], out_hbm.at[:, at], out_sem.at[c])
        store.start()
        stores.append(store)

    def finish_halo(side):
        for c in range(CHUNKS):
            for copy in halo_copies(c, side):
                copy.wait_send()

    pl.when(me < n - 1)(lambda: finish_halo(0))
    pl.when(me > 0)(lambda: finish_halo(1))
    for store in stores:
        store.wait()


def local(n, height, zonal_courant, merid_courant, rates, thresholds, flags, cutoffs):
    rows, levels, nlon = height.shape
    table, row_sum = latitude_table(rows * n)
    quarter_t, half_t = filter_tables(nlon)
    smem = pl.BlockSpec(memory_space=pltpu.SMEM)
    vmem = pl.BlockSpec(memory_space=pltpu.VMEM)
    hbm = pl.BlockSpec(memory_space=pl.ANY)
    block = pltpu.VMEM(height.shape, F32)
    return pl.pallas_call(
        functools.partial(kernel, n, nlon * row_sum),
        out_shape=jax.ShapeDtypeStruct(height.shape, F32),
        in_specs=[smem] * 3 + [vmem] * 2 + [hbm] * 5,
        out_specs=hbm,
        scratch_shapes=[
            block, block, block,
            pltpu.VMEM(quarter_t.shape, BF),
            pltpu.VMEM(half_t.shape, BF),
            block, block,
            pltpu.VMEM((2, levels, 128), F32),
            pltpu.VMEM((levels, 128), F32),
            pltpu.VMEM((1, 128), F32),
            pltpu.VMEM((n - 1, 1, 128), F32),
            pltpu.VMEM((2, levels, nlon), F32),
            pltpu.VMEM((levels, nlon), F32),
            pltpu.VMEM((2, levels, nlon), F32),
            pltpu.VMEM((levels, nlon), F32),
            pltpu.SemaphoreType.DMA((5,)),
            pltpu.SemaphoreType.DMA((CHUNKS,)),
            pltpu.SemaphoreType.DMA((2, CHUNKS, 2)),
            pltpu.SemaphoreType.DMA((2, CHUNKS, 2)),
            pltpu.SemaphoreType.DMA((n - 1,)),
            pltpu.SemaphoreType.DMA((n - 1,)),
        ],
        compiler_params=pltpu.CompilerParams(
            collective_id=0, has_side_effects=True, vmem_limit_bytes=48 * 1024 * 1024
        ),
    )(
        jnp.asarray(table), flags, cutoffs, rates[None, :], thresholds[None, :],
        height, zonal_courant, merid_courant, jnp.asarray(quarter_t), jnp.asarray(half_t),
    )


def solution(mesh):
    return jax.shard_map(
        functools.partial(local, mesh.shape["lat"]),
        mesh=mesh,
        in_specs=(
            P(("member", "lat"), None, None),
            P(("member", "lat"), None, None),
            P(("member", "lat"), None, None),
            P("member"),
            P("member"),
            P(),
            P(),
        ),
        out_specs=P(("member", "lat"), None, None),
        check_vma=False,
    )
```

```python
import functools

import jax
import jax.numpy as jnp
import numpy as np
from jax import lax
from jax.experimental import pallas as pl
from jax.experimental.pallas import tpu as pltpu
from jax.sharding import PartitionSpec as P

CHUNKS = 2
GROUP = 8
BF = jnp.bfloat16
F32 = jnp.float32


def split_table(table):
    high = table.astype(jnp.bfloat16)
    low = (table - high.astype(np.float64)).astype(jnp.bfloat16)
    return np.stack([high, low])


def cas(angle):
    return np.cos(angle) + np.sin(angle)


def filter_tables(nlon):
    quarter, half = nlon // 4, nlon // 2
    m = np.arange(quarter)
    zero = cas(2 * np.pi * (np.outer(m, m) % quarter) / quarter)
    odd = 2 * np.arange(half) + 1
    two = cas(2 * np.pi * (np.outer(odd[:quarter], odd[:quarter]) % nlon) / nlon)
    ones = cas(np.pi * (np.outer(odd, odd) % (2 * nlon)) / nlon)
    return split_table(np.stack([zero, two], 0)), split_table(ones)


def latitude_table(nlat):
    rows = np.sin(np.pi * (np.arange(nlat) + 0.5) / nlat)
    faces = np.sin(np.pi * np.arange(nlat + 1) / nlat)
    faces[0] = faces[-1] = 0.0
    table = np.concatenate([faces / 24.0, rows, 1.0 / rows]).astype(np.float32)
    return table, float(np.sum(rows))


def shifted(x, s):
    return jnp.concatenate([x[:, s:], x[:, :s]], axis=1)


def halves(x):
    high = x.astype(BF)
    return high, (x - high.astype(F32)).astype(BF)


def product(x, high_table, low_table):
    high, low = halves(x)
    rows = x.shape[0]
    both = jnp.dot(
        jnp.concatenate([high, low], axis=0), high_table, preferred_element_type=F32
    )
    return both[:rows] + both[rows:] + jnp.dot(high, low_table, preferred_element_type=F32)


def kernel(
    n, area,
    lat_hbm, flags_hbm, cutoffs_hbm, rates_hbm, thresholds_hbm,
    h_hbm, z_hbm, m_hbm, quarter_hbm, half_hbm,
    out_hbm,
    lat_ref, flags_ref, cutoffs_ref, rates_ref, thresholds_ref,
    h, z, m, quarter_t, half_t, base, result, sides, part, mine, others,
    hl, ml, hr, mr,
    in_sem, out_sem, halo_send, halo_recv, sum_send, sum_recv,
):
    rows, levels, nlon = h.shape
    me = lax.axis_index("lat")
    first = me * rows
    groups = levels // GROUP
    width = levels // CHUNKS

    loads = [
        pltpu.make_async_copy(src, dst, in_sem.at[i])
        for i, (src, dst) in enumerate(
            [
                (h_hbm, h), (z_hbm, z), (m_hbm, m), (quarter_hbm, quarter_t), (half_hbm, half_t),
                (lat_hbm, lat_ref), (flags_hbm, flags_ref), (cutoffs_hbm, cutoffs_ref),
                (rates_hbm, rates_ref), (thresholds_hbm, thresholds_ref),
            ]
        )
    ]
    for i in (0, 2, 1, 5, 6, 7, 8, 9):
        loads[i].start()
    nlat = rows * n

    def face_scale(f):
        return lat_ref[first + f]

    def row_weight(r):
        return lat_ref[nlat + 1 + first + r]

    def row_scale(r):
        return lat_ref[2 * nlat + 1 + first + r]

    barrier = pltpu.get_barrier_semaphore()

    def greet(o, c):
        pl.semaphore_signal(barrier, inc=1, device_id={"lat": lax.rem(me + o, n)})
        return c

    lax.fori_loop(1, n, greet, 0)
    pl.semaphore_wait(barrier, n - 1)

    def halo_copies(c, side):
        at = pl.ds(c * width, width)
        if side == 0:
            pairs = [
                (h.at[pl.ds(rows - 2, 2), at], hl.at[:, at]),
                (m.at[rows - 1, at], ml.at[at]),
            ]
            target = me + 1
        else:
            pairs = [
                (h.at[pl.ds(0, 2), at], hr.at[:, at]),
                (m.at[0, at], mr.at[at]),
            ]
            target = me - 1
        return [
            pltpu.make_async_remote_copy(
                src, dst, halo_send.at[side, c, i], halo_recv.at[side, c, i],
                device_id={"lat": target},
            )
            for i, (src, dst) in enumerate(pairs)
        ]

    def start_halo(side):
        for c in range(CHUNKS):
            for copy in halo_copies(c, side):
                copy.start()

    loads[0].wait()
    loads[2].wait()
    pl.when(me < n - 1)(lambda: start_halo(0))
    pl.when(me > 0)(lambda: start_halo(1))
    loads[3].start()
    loads[4].start()

    @pl.when(me == 0)
    def _():
        hl[...] = jnp.zeros_like(hl)
        ml[...] = jnp.zeros_like(ml)

    @pl.when(me == n - 1)
    def _():
        hr[...] = jnp.zeros_like(hr)
        mr[...] = jnp.zeros_like(mr)

    lane = lax.broadcasted_iota(jnp.int32, (levels, levels), 1)
    diagonal = lane == lax.broadcasted_iota(jnp.int32, (levels, levels), 0)

    def column(row):
        spread = jnp.where(diagonal, jnp.broadcast_to(row, (levels, levels)), 0.0)
        return jnp.sum(spread, axis=1, keepdims=True)

    for i in (5, 6, 7, 8, 9):
        loads[i].wait()
    sides[0] = jnp.broadcast_to(column(rates_ref[...]), (levels, 128))
    sides[1] = jnp.broadcast_to(column(thresholds_ref[...]), (levels, 128))

    loads[1].wait()

    def local_terms(g, carry):
        at = pl.ds(pl.multiple_of(g * GROUP, GROUP), GROUP)
        rate = sides[0, at, :][:, :1]
        threshold = sides[1, at, :][:, :1]
        weighted = jnp.zeros((GROUP, nlon), F32)
        for r in range(rows):
            hh = h[r, at, :]
            zz = z[r, at, :]
            face = 7.0 * (hh + shifted(hh, 1)) - (shifted(hh, nlon - 1) + shifted(hh, 2))
            flux = (zz + shifted(zz, 1)) * face * (1.0 / 24.0)
            source = -rate * jnp.log(1.0 + jnp.exp(hh - threshold))
            base[r, at, :] = hh - (flux - shifted(flux, nlon - 1)) + source
            weighted = weighted + source * row_weight(r)
        total = jnp.sum(weighted, axis=1, keepdims=True)
        part[at, :] = jnp.broadcast_to(total, (GROUP, 128))
        return carry

    lax.fori_loop(0, groups, local_terms, 0)

    wide = lax.broadcasted_iota(jnp.int32, (levels, 128), 1)
    tall = lax.broadcasted_iota(jnp.int32, (levels, 128), 0)
    mine[...] = jnp.sum(jnp.where(wide == tall, part[...], 0.0), axis=0, keepdims=True)

    def sum_copy(o):
        return pltpu.make_async_remote_copy(
            mine, others.at[o - 1], sum_send.at[o - 1], sum_recv.at[o - 1],
            device_id={"lat": lax.rem(me + o, n)},
        )

    def send_sum(o, c):
        sum_copy(o).start()
        return c

    lax.fori_loop(1, n, send_sum, 0)

    quarter, half = nlon // 4, nlon // 2

    def factors(length, step, offset):
        k = lax.broadcasted_iota(jnp.int32, (1, length), 1) * step + offset
        k = jnp.maximum(jnp.minimum(k, nlon - k), 1).astype(F32)
        out = []
        for r in range(rows):
            ratio = cutoffs_ref[first + r].astype(F32) / k
            factor = (1.0 - jnp.minimum(1.0, ratio * ratio)) * (1.0 / nlon)
            on = jnp.where(flags_ref[first + r] > 0, 1.0, 0.0)
            out.append(factor * on)
        return out

    all_factors = [factors(quarter, 4, 0), factors(quarter, 4, 2), factors(half, 2, 1)]

    def removed(x, high_table, low_table, factor):
        spectrum = product(x, high_table, low_table).reshape(rows, width, x.shape[1])
        scaled = jnp.concatenate([spectrum[r] * factor[r] for r in range(rows)], axis=0)
        return product(scaled, high_table, low_table)

    polar = jnp.logical_or(first < nlat // 4, first + rows > nlat - nlat // 4)

    def merid(c):
        def body(g, carry):
            at = pl.ds(pl.multiple_of(c * width + g * GROUP, GROUP), GROUP)

            def height(i):
                return hl[i + 2, at, :] if i < 0 else hr[i - rows, at, :] if i >= rows else h[i, at, :]

            def speed(i):
                return ml[at, :] if i < 0 else mr[at, :] if i >= rows else m[i, at, :]

            previous = None
            for f in range(rows + 1):
                face = 7.0 * (height(f - 1) + height(f)) - (height(f - 2) + height(f + 1))
                flux = (speed(f - 1) + speed(f)) * face * face_scale(f)
                if f > 0:
                    base[f - 1, at, :] -= (flux - previous) * row_scale(f - 1)
                previous = flux
            return carry

        lax.fori_loop(0, width // GROUP, body, 0)

    mean = None
    stores = []
    for c in range(CHUNKS):
        @pl.when(me > 0)
        def _():
            for copy in halo_copies(c, 0):
                copy.wait_recv()

        @pl.when(me < n - 1)
        def _():
            for copy in halo_copies(c, 1):
                copy.wait_recv()

        merid(c)
        if c == 0:
            loads[3].wait()
            loads[4].wait()
        if c == 0:
            def wait_sum(o, carry):
                sum_copy(o).wait()
                return carry

            lax.fori_loop(1, n, wait_sum, 0)
            total = mine[...] + jnp.sum(others[...], axis=0)
            mean = column(total[:, :levels]) * (1.0 / area)
        at = pl.ds(c * width, width)
        level_mean = mean[c * width : (c + 1) * width][None]

        @pl.when(polar)
        def _():
            x = base[:, at, :].reshape(rows * width, nlon)
            near, far = x[:, :half], x[:, half:]
            even, odd = near + far, near - far
            left, right = even[:, :quarter], even[:, quarter:]
            zero = removed(left + right, quarter_t[0, 0], quarter_t[1, 0], all_factors[0])
            two = removed(left - right, quarter_t[0, 1], quarter_t[1, 1], all_factors[1])
            ones = removed(odd, half_t[0], half_t[1], all_factors[2])
            even = jnp.concatenate([zero + two, zero - two], axis=1)
            kept = jnp.concatenate([near - even - ones, far - even + ones], axis=1)
            result[:, at, :] = kept.reshape(rows, width, nlon) - level_mean

        @pl.when(jnp.logical_not(polar))
        def _():
            result[:, at, :] = base[:, at, :] - level_mean

        store = pltpu.make_async_copy(result.at[:, at], out_hbm.at[:, at], out_sem.at[c])
        store.start()
        stores.append(store)

    def finish_halo(side):
        for c in range(CHUNKS):
            for copy in halo_copies(c, side):
                copy.wait_send()

    pl.when(me < n - 1)(lambda: finish_halo(0))
    pl.when(me > 0)(lambda: finish_halo(1))
    for store in stores:
        store.wait()


def local(n, height, zonal_courant, merid_courant, rates, thresholds, flags, cutoffs):
    rows, levels, nlon = height.shape
    table, row_sum = latitude_table(rows * n)
    quarter_t, half_t = filter_tables(nlon)
    hbm = pl.BlockSpec(memory_space=pltpu.HBM)
    any_space = pl.BlockSpec(memory_space=pl.ANY)
    block = pltpu.VMEM(height.shape, F32)
    return pl.pallas_call(
        functools.partial(kernel, n, nlon * row_sum),
        out_shape=jax.ShapeDtypeStruct(height.shape, F32),
        in_specs=[hbm] * 10,
        out_specs=any_space,
        scratch_shapes=[
            pltpu.SMEM(table.shape, F32),
            pltpu.SMEM(flags.shape, jnp.int32),
            pltpu.SMEM(cutoffs.shape, jnp.int32),
            pltpu.VMEM((1, levels), F32),
            pltpu.VMEM((1, levels), F32),
            block, block, block,
            pltpu.VMEM(quarter_t.shape, BF),
            pltpu.VMEM(half_t.shape, BF),
            block, block,
            pltpu.VMEM((2, levels, 128), F32),
            pltpu.VMEM((levels, 128), F32),
            pltpu.VMEM((1, 128), F32),
            pltpu.VMEM((n - 1, 1, 128), F32),
            pltpu.VMEM((2, levels, nlon), F32),
            pltpu.VMEM((levels, nlon), F32),
            pltpu.VMEM((2, levels, nlon), F32),
            pltpu.VMEM((levels, nlon), F32),
            pltpu.SemaphoreType.DMA((10,)),
            pltpu.SemaphoreType.DMA((CHUNKS,)),
            pltpu.SemaphoreType.DMA((2, CHUNKS, 2)),
            pltpu.SemaphoreType.DMA((2, CHUNKS, 2)),
            pltpu.SemaphoreType.DMA((n - 1,)),
            pltpu.SemaphoreType.DMA((n - 1,)),
        ],
        compiler_params=pltpu.CompilerParams(
            collective_id=0, has_side_effects=True, vmem_limit_bytes=67043328
        ),
    )(
        jnp.asarray(table), flags, cutoffs, rates[None, :], thresholds[None, :],
        height, zonal_courant, merid_courant, jnp.asarray(quarter_t), jnp.asarray(half_t),
    )


def solution(mesh):
    return jax.shard_map(
        functools.partial(local, mesh.shape["lat"]),
        mesh=mesh,
        in_specs=(
            P(("member", "lat"), None, None),
            P(("member", "lat"), None, None),
            P(("member", "lat"), None, None),
            P("member"),
            P("member"),
            P(),
            P(),
        ),
        out_specs=P(("member", "lat"), None, None),
        check_vma=False,
    )
```

```python
import functools

import jax
import jax.numpy as jnp
import numpy as np
from jax import lax
from jax.experimental import pallas as pl
from jax.experimental.pallas import tpu as pltpu
from jax.sharding import PartitionSpec as P

CHUNKS = 2
GROUP = 8
BF = jnp.bfloat16
F32 = jnp.float32


def split_table(table):
    high = table.astype(jnp.bfloat16)
    low = (table - high.astype(np.float64)).astype(jnp.bfloat16)
    return np.stack([high, low])


def cas(angle):
    return np.cos(angle) + np.sin(angle)


def filter_tables(nlon):
    quarter, half = nlon // 4, nlon // 2
    m = np.arange(quarter)
    zero = cas(2 * np.pi * (np.outer(m, m) % quarter) / quarter)
    odd = 2 * np.arange(half) + 1
    two = cas(2 * np.pi * (np.outer(odd[:quarter], odd[:quarter]) % nlon) / nlon)
    ones = cas(np.pi * (np.outer(odd, odd) % (2 * nlon)) / nlon)
    return split_table(np.stack([zero, two], 0)), split_table(ones)


def latitude_table(nlat):
    rows = np.sin(np.pi * (np.arange(nlat) + 0.5) / nlat)
    faces = np.sin(np.pi * np.arange(nlat + 1) / nlat)
    faces[0] = faces[-1] = 0.0
    table = np.concatenate([faces / 24.0, rows, 1.0 / rows]).astype(np.float32)
    return table, float(np.sum(rows))


def shifted(x, s):
    return jnp.concatenate([x[:, s:], x[:, :s]], axis=1)


def halves(x):
    high = x.astype(BF)
    return high, (x - high.astype(F32)).astype(BF)


def product(x, high_table, low_table):
    high, low = halves(x)
    rows = x.shape[0]
    both = jnp.dot(
        jnp.concatenate([high, low], axis=0), high_table, preferred_element_type=F32
    )
    return both[:rows] + both[rows:] + jnp.dot(high, low_table, preferred_element_type=F32)


def kernel(
    n, area,
    lat_hbm, flags_hbm, cutoffs_hbm, rates_hbm, thresholds_hbm,
    h_hbm, z_hbm, m_hbm, quarter_hbm, half_hbm,
    out,
    lat_ref, flags_ref, cutoffs_ref, rates_ref, thresholds_ref,
    h, z, m, quarter_t, half_t, base, sides, part, mine, others,
    hl, ml, hr, mr,
    in_sem, halo_send, halo_recv, sum_send, sum_recv,
):
    rows, levels, nlon = h.shape
    me = lax.axis_index("lat")
    first = me * rows
    groups = levels // GROUP
    width = levels // CHUNKS

    loads = [
        pltpu.make_async_copy(src, dst, in_sem.at[i])
        for i, (src, dst) in enumerate(
            [
                (h_hbm, h), (z_hbm, z), (m_hbm, m), (quarter_hbm, quarter_t), (half_hbm, half_t),
                (lat_hbm, lat_ref), (flags_hbm, flags_ref), (cutoffs_hbm, cutoffs_ref),
                (rates_hbm, rates_ref), (thresholds_hbm, thresholds_ref),
            ]
        )
    ]
    for i in (0, 2, 1, 5, 6, 7, 8, 9):
        loads[i].start()
    nlat = rows * n

    def face_scale(f):
        return lat_ref[first + f]

    def row_weight(r):
        return lat_ref[nlat + 1 + first + r]

    def row_scale(r):
        return lat_ref[2 * nlat + 1 + first + r]

    barrier = pltpu.get_barrier_semaphore()

    def greet(o, c):
        pl.semaphore_signal(barrier, inc=1, device_id={"lat": lax.rem(me + o, n)})
        return c

    lax.fori_loop(1, n, greet, 0)
    pl.semaphore_wait(barrier, n - 1)

    def halo_copies(c, side):
        at = pl.ds(c * width, width)
        if side == 0:
            pairs = [
                (h.at[pl.ds(rows - 2, 2), at], hl.at[:, at]),
                (m.at[rows - 1, at], ml.at[at]),
            ]
            target = me + 1
        else:
            pairs = [
                (h.at[pl.ds(0, 2), at], hr.at[:, at]),
                (m.at[0, at], mr.at[at]),
            ]
            target = me - 1
        return [
            pltpu.make_async_remote_copy(
                src, dst, halo_send.at[side, c, i], halo_recv.at[side, c, i],
                device_id={"lat": target},
            )
            for i, (src, dst) in enumerate(pairs)
        ]

    def start_halo(side):
        for c in range(CHUNKS):
            for copy in halo_copies(c, side):
                copy.start()

    loads[0].wait()
    loads[2].wait()
    pl.when(me < n - 1)(lambda: start_halo(0))
    pl.when(me > 0)(lambda: start_halo(1))
    loads[3].start()
    loads[4].start()

    @pl.when(me == 0)
    def _():
        hl[...] = jnp.zeros_like(hl)
        ml[...] = jnp.zeros_like(ml)

    @pl.when(me == n - 1)
    def _():
        hr[...] = jnp.zeros_like(hr)
        mr[...] = jnp.zeros_like(mr)

    lane = lax.broadcasted_iota(jnp.int32, (levels, levels), 1)
    diagonal = lane == lax.broadcasted_iota(jnp.int32, (levels, levels), 0)

    def column(row):
        spread = jnp.where(diagonal, jnp.broadcast_to(row, (levels, levels)), 0.0)
        return jnp.sum(spread, axis=1, keepdims=True)

    for i in (5, 6, 7, 8, 9):
        loads[i].wait()
    sides[0] = jnp.broadcast_to(column(rates_ref[...]), (levels, 128))
    sides[1] = jnp.broadcast_to(column(thresholds_ref[...]), (levels, 128))

    loads[1].wait()

    def local_terms(g, carry):
        at = pl.ds(pl.multiple_of(g * GROUP, GROUP), GROUP)
        rate = sides[0, at, :][:, :1]
        threshold = sides[1, at, :][:, :1]
        weighted = jnp.zeros((GROUP, nlon), F32)
        for r in range(rows):
            hh = h[r, at, :]
            zz = z[r, at, :]
            face = 7.0 * (hh + shifted(hh, 1)) - (shifted(hh, nlon - 1) + shifted(hh, 2))
            flux = (zz + shifted(zz, 1)) * face * (1.0 / 24.0)
            source = -rate * jnp.log(1.0 + jnp.exp(hh - threshold))
            base[r, at, :] = hh - (flux - shifted(flux, nlon - 1)) + source
            weighted = weighted + source * row_weight(r)
        total = jnp.sum(weighted, axis=1, keepdims=True)
        part[at, :] = jnp.broadcast_to(total, (GROUP, 128))
        return carry

    lax.fori_loop(0, groups, local_terms, 0)

    wide = lax.broadcasted_iota(jnp.int32, (levels, 128), 1)
    tall = lax.broadcasted_iota(jnp.int32, (levels, 128), 0)
    mine[...] = jnp.sum(jnp.where(wide == tall, part[...], 0.0), axis=0, keepdims=True)

    def sum_copy(o):
        return pltpu.make_async_remote_copy(
            mine, others.at[o - 1], sum_send.at[o - 1], sum_recv.at[o - 1],
            device_id={"lat": lax.rem(me + o, n)},
        )

    def send_sum(o, c):
        sum_copy(o).start()
        return c

    lax.fori_loop(1, n, send_sum, 0)

    quarter, half = nlon // 4, nlon // 2

    def factors(length, step, offset):
        k = lax.broadcasted_iota(jnp.int32, (1, length), 1) * step + offset
        k = jnp.maximum(jnp.minimum(k, nlon - k), 1).astype(F32)
        out = []
        for r in range(rows):
            ratio = cutoffs_ref[first + r].astype(F32) / k
            factor = (1.0 - jnp.minimum(1.0, ratio * ratio)) * (1.0 / nlon)
            on = jnp.where(flags_ref[first + r] > 0, 1.0, 0.0)
            out.append(factor * on)
        return out

    all_factors = [factors(quarter, 4, 0), factors(quarter, 4, 2), factors(half, 2, 1)]

    def removed(x, high_table, low_table, factor):
        spectrum = product(x, high_table, low_table).reshape(rows, width, x.shape[1])
        scaled = jnp.concatenate([spectrum[r] * factor[r] for r in range(rows)], axis=0)
        return product(scaled, high_table, low_table)

    polar = jnp.logical_or(first < nlat // 4, first + rows > nlat - nlat // 4)

    def merid(c):
        def body(g, carry):
            at = pl.ds(pl.multiple_of(c * width + g * GROUP, GROUP), GROUP)

            def height(i):
                return hl[i + 2, at, :] if i < 0 else hr[i - rows, at, :] if i >= rows else h[i, at, :]

            def speed(i):
                return ml[at, :] if i < 0 else mr[at, :] if i >= rows else m[i, at, :]

            previous = None
            for f in range(rows + 1):
                face = 7.0 * (height(f - 1) + height(f)) - (height(f - 2) + height(f + 1))
                flux = (speed(f - 1) + speed(f)) * face * face_scale(f)
                if f > 0:
                    base[f - 1, at, :] -= (flux - previous) * row_scale(f - 1)
                previous = flux
            return carry

        lax.fori_loop(0, width // GROUP, body, 0)

    mean = None
    for c in range(CHUNKS):
        @pl.when(me > 0)
        def _():
            for copy in halo_copies(c, 0):
                copy.wait_recv()

        @pl.when(me < n - 1)
        def _():
            for copy in halo_copies(c, 1):
                copy.wait_recv()

        merid(c)
        if c == 0:
            loads[3].wait()
            loads[4].wait()
        if c == 0:
            def wait_sum(o, carry):
                sum_copy(o).wait()
                return carry

            lax.fori_loop(1, n, wait_sum, 0)
            total = mine[...] + jnp.sum(others[...], axis=0)
            mean = column(total[:, :levels]) * (1.0 / area)
        at = pl.ds(c * width, width)
        level_mean = mean[c * width : (c + 1) * width][None]

        @pl.when(polar)
        def _():
            x = base[:, at, :].reshape(rows * width, nlon)
            near, far = x[:, :half], x[:, half:]
            even, odd = near + far, near - far
            left, right = even[:, :quarter], even[:, quarter:]
            zero = removed(left + right, quarter_t[0, 0], quarter_t[1, 0], all_factors[0])
            two = removed(left - right, quarter_t[0, 1], quarter_t[1, 1], all_factors[1])
            ones = removed(odd, half_t[0], half_t[1], all_factors[2])
            even = jnp.concatenate([zero + two, zero - two], axis=1)
            kept = jnp.concatenate([near - even - ones, far - even + ones], axis=1)
            out[:, at, :] = kept.reshape(rows, width, nlon) - level_mean

        @pl.when(jnp.logical_not(polar))
        def _():
            out[:, at, :] = base[:, at, :] - level_mean


    def finish_halo(side):
        for c in range(CHUNKS):
            for copy in halo_copies(c, side):
                copy.wait_send()

    pl.when(me < n - 1)(lambda: finish_halo(0))
    pl.when(me > 0)(lambda: finish_halo(1))


def local(n, height, zonal_courant, merid_courant, rates, thresholds, flags, cutoffs):
    rows, levels, nlon = height.shape
    table, row_sum = latitude_table(rows * n)
    quarter_t, half_t = filter_tables(nlon)
    hbm = pl.BlockSpec(memory_space=pltpu.HBM)
    vmem = pl.BlockSpec(memory_space=pltpu.VMEM)
    block = pltpu.VMEM(height.shape, F32)
    return pl.pallas_call(
        functools.partial(kernel, n, nlon * row_sum),
        out_shape=pltpu.VMEM(height.shape, F32),
        in_specs=[hbm] * 10,
        out_specs=vmem,
        scratch_shapes=[
            pltpu.SMEM(table.shape, F32),
            pltpu.SMEM(flags.shape, jnp.int32),
            pltpu.SMEM(cutoffs.shape, jnp.int32),
            pltpu.VMEM((1, levels), F32),
            pltpu.VMEM((1, levels), F32),
            block, block, block,
            pltpu.VMEM(quarter_t.shape, BF),
            pltpu.VMEM(half_t.shape, BF),
            block,
            pltpu.VMEM((2, levels, 128), F32),
            pltpu.VMEM((levels, 128), F32),
            pltpu.VMEM((1, 128), F32),
            pltpu.VMEM((n - 1, 1, 128), F32),
            pltpu.VMEM((2, levels, nlon), F32),
            pltpu.VMEM((levels, nlon), F32),
            pltpu.VMEM((2, levels, nlon), F32),
            pltpu.VMEM((levels, nlon), F32),
            pltpu.SemaphoreType.DMA((10,)),
            pltpu.SemaphoreType.DMA((2, CHUNKS, 2)),
            pltpu.SemaphoreType.DMA((2, CHUNKS, 2)),
            pltpu.SemaphoreType.DMA((n - 1,)),
            pltpu.SemaphoreType.DMA((n - 1,)),
        ],
        compiler_params=pltpu.CompilerParams(
            collective_id=0, has_side_effects=True, vmem_limit_bytes=62 * 1024 * 1024
        ),
    )(
        jnp.asarray(table), flags, cutoffs, rates[None, :], thresholds[None, :],
        height, zonal_courant, merid_courant, jnp.asarray(quarter_t), jnp.asarray(half_t),
    )


def solution(mesh):
    return jax.shard_map(
        functools.partial(local, mesh.shape["lat"]),
        mesh=mesh,
        in_specs=(
            P(("member", "lat"), None, None),
            P(("member", "lat"), None, None),
            P(("member", "lat"), None, None),
            P("member"),
            P("member"),
            P(),
            P(),
        ),
        out_specs=P(("member", "lat"), None, None),
        check_vma=False,
    )
```

```python
import functools

import jax
import jax.numpy as jnp
import numpy as np
from jax import lax
from jax.experimental import pallas as pl
from jax.experimental.pallas import tpu as pltpu
from jax.sharding import PartitionSpec as P

CHUNKS = 4
IN_FLIGHT = 3
FILTERED = ((0, 3), (3, 4))
GROUP = 8
BF = jnp.bfloat16
F32 = jnp.float32


def split_table(table):
    high = table.astype(jnp.bfloat16)
    low = (table - high.astype(np.float64)).astype(jnp.bfloat16)
    return np.stack([high, low])


def cas(angle):
    return np.cos(angle) + np.sin(angle)


def filter_tables(nlon):
    quarter, half = nlon // 4, nlon // 2
    m = np.arange(quarter)
    zero = cas(2 * np.pi * (np.outer(m, m) % quarter) / quarter)
    odd = 2 * np.arange(half) + 1
    two = cas(2 * np.pi * (np.outer(odd[:quarter], odd[:quarter]) % nlon) / nlon)
    ones = cas(np.pi * (np.outer(odd, odd) % (2 * nlon)) / nlon)
    return split_table(np.stack([zero, two], 0)), split_table(ones)


def latitude_table(nlat):
    rows = np.sin(np.pi * (np.arange(nlat) + 0.5) / nlat)
    faces = np.sin(np.pi * np.arange(nlat + 1) / nlat)
    faces[0] = faces[-1] = 0.0
    table = np.concatenate([faces / 24.0, rows, 1.0 / rows]).astype(np.float32)
    return table, float(np.sum(rows))


def shifted(x, s):
    return jnp.concatenate([x[:, s:], x[:, :s]], axis=1)


def halves(x):
    high = x.astype(BF)
    return high, (x - high.astype(F32)).astype(BF)


def product(x, high_table, low_table):
    high, low = halves(x)
    rows = x.shape[0]
    both = jnp.dot(
        jnp.concatenate([high, low], axis=0), high_table, preferred_element_type=F32
    )
    return both[:rows] + both[rows:] + jnp.dot(high, low_table, preferred_element_type=F32)


def kernel(
    n, area,
    lat_hbm, flags_hbm, cutoffs_hbm, rates_hbm, thresholds_hbm,
    h_hbm, z_hbm, m_hbm, quarter_hbm, half_hbm,
    out,
    lat_ref, flags_ref, cutoffs_ref, rates_ref, thresholds_ref,
    h, z, m, quarter_t, half_t, base, sides, part, mine, others,
    hl, ml, hr, mr,
    in_sem, halo_send, halo_recv, sum_send, sum_recv,
):
    rows, levels, nlon = h.shape
    me = lax.axis_index("lat")
    first = me * rows
    groups = levels // GROUP
    width = levels // CHUNKS

    loads = [
        pltpu.make_async_copy(src, dst, in_sem.at[i])
        for i, (src, dst) in enumerate(
            [
                (h_hbm, h), (z_hbm, z), (m_hbm, m), (quarter_hbm, quarter_t), (half_hbm, half_t),
                (lat_hbm, lat_ref), (flags_hbm, flags_ref), (cutoffs_hbm, cutoffs_ref),
                (rates_hbm, rates_ref), (thresholds_hbm, thresholds_ref),
            ]
        )
    ]
    for i in (0, 2, 1, 5, 6, 7, 8, 9):
        loads[i].start()
    nlat = rows * n

    def face_scale(f):
        return lat_ref[first + f]

    def row_weight(r):
        return lat_ref[nlat + 1 + first + r]

    def row_scale(r):
        return lat_ref[2 * nlat + 1 + first + r]

    barrier = pltpu.get_barrier_semaphore()

    def in_group(o):
        return me - lax.rem(me, 4) + lax.rem(me + o, 4)


    for o in (1, 2, 3):
        pl.semaphore_signal(barrier, inc=1, device_id={"lat": in_group(o)})
    for o in range(4, n, 4):
        pl.semaphore_signal(barrier, inc=1, device_id={"lat": lax.rem(me + o, n)})
    up = jnp.logical_and(lax.rem(me, 4) == 3, me < n - 1)
    down = jnp.logical_and(lax.rem(me, 4) == 0, me > 0)
    pl.when(up)(lambda: pl.semaphore_signal(barrier, inc=1, device_id={"lat": me + 1}))
    pl.when(down)(lambda: pl.semaphore_signal(barrier, inc=1, device_id={"lat": me - 1}))
    pl.semaphore_wait(barrier, 2 + n // 4 + up.astype(jnp.int32) + down.astype(jnp.int32))

    def halo_copies(c, side):
        at = pl.ds(c * width, width)
        if side == 0:
            pairs = [
                (h.at[pl.ds(rows - 2, 2), at], hl.at[:, at]),
                (m.at[rows - 1, at], ml.at[at]),
            ]
            target = me + 1
        else:
            pairs = [
                (h.at[pl.ds(0, 2), at], hr.at[:, at]),
                (m.at[0, at], mr.at[at]),
            ]
            target = me - 1
        return [
            pltpu.make_async_remote_copy(
                src, dst, halo_send.at[side, c, i], halo_recv.at[side, c, i],
                device_id={"lat": target},
            )
            for i, (src, dst) in enumerate(pairs)
        ]

    def each(side, chunks, act):
        @pl.when(me < n - 1 if side == 0 else me > 0)
        def _():
            for c in chunks:
                for copy in halo_copies(c, side):
                    act(copy)

    def start_halo(chunks):
        each(0, chunks, lambda copy: copy.start())
        each(1, chunks, lambda copy: copy.start())

    loads[0].wait()
    loads[2].wait()
    start_halo(range(IN_FLIGHT))
    loads[3].start()
    loads[4].start()

    @pl.when(me == 0)
    def _():
        hl[...] = jnp.zeros_like(hl)
        ml[...] = jnp.zeros_like(ml)

    @pl.when(me == n - 1)
    def _():
        hr[...] = jnp.zeros_like(hr)
        mr[...] = jnp.zeros_like(mr)

    lane = lax.broadcasted_iota(jnp.int32, (levels, levels), 1)
    diagonal = lane == lax.broadcasted_iota(jnp.int32, (levels, levels), 0)

    def column(row):
        spread = jnp.where(diagonal, jnp.broadcast_to(row, (levels, levels)), 0.0)
        return jnp.sum(spread, axis=1, keepdims=True)

    for i in (5, 6, 7, 8, 9):
        loads[i].wait()
    sides[0] = jnp.broadcast_to(column(rates_ref[...]), (levels, 128))
    sides[1] = jnp.broadcast_to(column(thresholds_ref[...]), (levels, 128))

    loads[1].wait()

    def local_terms(g, carry):
        at = pl.ds(pl.multiple_of(g * GROUP, GROUP), GROUP)
        rate = sides[0, at, :][:, :1]
        threshold = sides[1, at, :][:, :1]
        weighted = jnp.zeros((GROUP, nlon), F32)
        for r in range(rows):
            hh = h[r, at, :]
            zz = z[r, at, :]
            face = 7.0 * (hh + shifted(hh, 1)) - (shifted(hh, nlon - 1) + shifted(hh, 2))
            flux = (zz + shifted(zz, 1)) * face * (1.0 / 24.0)
            source = -rate * jnp.log(1.0 + jnp.exp(hh - threshold))
            base[r, at, :] = hh - (flux - shifted(flux, nlon - 1)) + source
            weighted = weighted + source * row_weight(r)
        total = jnp.sum(weighted, axis=1, keepdims=True)
        part[at, :] = jnp.broadcast_to(total, (GROUP, 128))
        return carry

    lax.fori_loop(0, groups, local_terms, 0)

    wide = lax.broadcasted_iota(jnp.int32, (levels, 128), 1)
    tall = lax.broadcasted_iota(jnp.int32, (levels, 128), 0)
    mine[0] = jnp.sum(jnp.where(wide == tall, part[...], 0.0), axis=0, keepdims=True)

    def sum_copy(stage, slot, target):
        return pltpu.make_async_remote_copy(
            mine.at[stage], others.at[slot], sum_send.at[slot], sum_recv.at[slot],
            device_id={"lat": target},
        )

    near_sums = [sum_copy(0, o - 1, in_group(o)) for o in (1, 2, 3)]
    far_sums = [sum_copy(1, 2 + o, lax.rem(me + 4 * o, n)) for o in range(1, n // 4)]
    for copy in near_sums:
        copy.start()

    quarter, half = nlon // 4, nlon // 2

    def factors(length, step, offset):
        k = lax.broadcasted_iota(jnp.int32, (1, length), 1) * step + offset
        k = jnp.maximum(jnp.minimum(k, nlon - k), 1).astype(F32)
        out = []
        for r in range(rows):
            ratio = cutoffs_ref[first + r].astype(F32) / k
            factor = (1.0 - jnp.minimum(1.0, ratio * ratio)) * (1.0 / nlon)
            on = jnp.where(flags_ref[first + r] > 0, 1.0, 0.0)
            out.append(factor * on)
        return out

    all_factors = [factors(quarter, 4, 0), factors(quarter, 4, 2), factors(half, 2, 1)]

    def removed(x, high_table, low_table, factor):
        spectrum = product(x, high_table, low_table).reshape(rows, -1, x.shape[1])
        scaled = jnp.concatenate([spectrum[r] * factor[r] for r in range(rows)], axis=0)
        return product(scaled, high_table, low_table)

    polar = jnp.logical_or(first < nlat // 4, first + rows > nlat - nlat // 4)

    def merid(c):
        def body(g, carry):
            at = pl.ds(pl.multiple_of(c * width + g * GROUP, GROUP), GROUP)

            def height(i):
                return hl[i + 2, at, :] if i < 0 else hr[i - rows, at, :] if i >= rows else h[i, at, :]

            def speed(i):
                return ml[at, :] if i < 0 else mr[at, :] if i >= rows else m[i, at, :]

            previous = None
            for f in range(rows + 1):
                face = 7.0 * (height(f - 1) + height(f)) - (height(f - 2) + height(f + 1))
                flux = (speed(f - 1) + speed(f)) * face * face_scale(f)
                if f > 0:
                    base[f - 1, at, :] -= (flux - previous) * row_scale(f - 1)
                previous = flux
            return carry

        lax.fori_loop(0, width // GROUP, body, 0)

    def receive(c):
        @pl.when(me > 0)
        def _():
            for copy in halo_copies(c, 0):
                copy.wait_recv()

        @pl.when(me < n - 1)
        def _():
            for copy in halo_copies(c, 1):
                copy.wait_recv()

        each(0, [c], lambda copy: copy.wait_send())
        each(1, [c], lambda copy: copy.wait_send())
        if c + IN_FLIGHT < CHUNKS:
            start_halo([c + IN_FLIGHT])

    mean = None
    for low, high in FILTERED:
        for c in range(low, high):
            receive(c)
            merid(c)
            if c == 0:
                for copy in near_sums:
                    copy.wait()
                mine[1] = mine[0] + jnp.sum(others[:3], axis=0)
                for copy in far_sums:
                    copy.start()
        if low == 0:
            loads[3].wait()
            loads[4].wait()
            for copy in far_sums:
                copy.wait()
            total = mine[1] + jnp.sum(others[3:], axis=0)
            mean = column(total[:, :levels]) * (1.0 / area)
        at = pl.ds(low * width, (high - low) * width)
        level_mean = mean[low * width : high * width][None]

        @pl.when(polar)
        def _():
            x = base[:, at, :].reshape(rows * (high - low) * width, nlon)
            near, far = x[:, :half], x[:, half:]
            even, odd = near + far, near - far
            left, right = even[:, :quarter], even[:, quarter:]
            zero = removed(left + right, quarter_t[0, 0], quarter_t[1, 0], all_factors[0])
            two = removed(left - right, quarter_t[0, 1], quarter_t[1, 1], all_factors[1])
            ones = removed(odd, half_t[0], half_t[1], all_factors[2])
            even = jnp.concatenate([zero + two, zero - two], axis=1)
            kept = jnp.concatenate([near - even - ones, far - even + ones], axis=1)
            out[:, at, :] = kept.reshape(rows, (high - low) * width, nlon) - level_mean

        @pl.when(jnp.logical_not(polar))
        def _():
            out[:, at, :] = base[:, at, :] - level_mean


def local(n, height, zonal_courant, merid_courant, rates, thresholds, flags, cutoffs):
    rows, levels, nlon = height.shape
    table, row_sum = latitude_table(rows * n)
    quarter_t, half_t = filter_tables(nlon)
    hbm = pl.BlockSpec(memory_space=pltpu.HBM)
    vmem = pl.BlockSpec(memory_space=pltpu.VMEM)
    block = pltpu.VMEM(height.shape, F32)
    return pl.pallas_call(
        functools.partial(kernel, n, nlon * row_sum),
        out_shape=pltpu.VMEM(height.shape, F32),
        in_specs=[hbm] * 10,
        out_specs=vmem,
        scratch_shapes=[
            pltpu.SMEM(table.shape, F32),
            pltpu.SMEM(flags.shape, jnp.int32),
            pltpu.SMEM(cutoffs.shape, jnp.int32),
            pltpu.VMEM((1, levels), F32),
            pltpu.VMEM((1, levels), F32),
            block, block, block,
            pltpu.VMEM(quarter_t.shape, BF),
            pltpu.VMEM(half_t.shape, BF),
            block,
            pltpu.VMEM((2, levels, 128), F32),
            pltpu.VMEM((levels, 128), F32),
            pltpu.VMEM((2, 1, 128), F32),
            pltpu.VMEM((2 + n // 4, 1, 128), F32),
            pltpu.VMEM((2, levels, nlon), F32),
            pltpu.VMEM((levels, nlon), F32),
            pltpu.VMEM((2, levels, nlon), F32),
            pltpu.VMEM((levels, nlon), F32),
            pltpu.SemaphoreType.DMA((10,)),
            pltpu.SemaphoreType.DMA((2, CHUNKS, 2)),
            pltpu.SemaphoreType.DMA((2, CHUNKS, 2)),
            pltpu.SemaphoreType.DMA((2 + n // 4,)),
            pltpu.SemaphoreType.DMA((2 + n // 4,)),
        ],
        compiler_params=pltpu.CompilerParams(
            collective_id=0, has_side_effects=True, vmem_limit_bytes=62 * 1024 * 1024
        ),
    )(
        jnp.asarray(table), flags, cutoffs, rates[None, :], thresholds[None, :],
        height, zonal_courant, merid_courant, jnp.asarray(quarter_t), jnp.asarray(half_t),
    )


def solution(mesh):
    return jax.shard_map(
        functools.partial(local, mesh.shape["lat"]),
        mesh=mesh,
        in_specs=(
            P(("member", "lat"), None, None),
            P(("member", "lat"), None, None),
            P(("member", "lat"), None, None),
            P("member"),
            P("member"),
            P(),
            P(),
        ),
        out_specs=P(("member", "lat"), None, None),
        check_vma=False,
    )
```

```python
import functools

import jax
import jax.numpy as jnp
import numpy as np
from jax import lax
from jax.experimental import pallas as pl
from jax.experimental.pallas import tpu as pltpu
from jax.sharding import PartitionSpec as P

CHUNKS = 4
IN_FLIGHT = 3
FILTERED = ((0, 2), (2, 4))
GROUP = 8
BF = jnp.bfloat16
F32 = jnp.float32


def split_table(table):
    high = table.astype(jnp.bfloat16)
    low = (table - high.astype(np.float64)).astype(jnp.bfloat16)
    return np.stack([high, low])


def cas(angle):
    return np.cos(angle) + np.sin(angle)


def filter_tables(nlon):
    quarter, half = nlon // 4, nlon // 2
    m = np.arange(quarter)
    zero = cas(2 * np.pi * (np.outer(m, m) % quarter) / quarter)
    odd = 2 * np.arange(half) + 1
    two = cas(2 * np.pi * (np.outer(odd[:quarter], odd[:quarter]) % nlon) / nlon)
    ones = cas(np.pi * (np.outer(odd, odd) % (2 * nlon)) / nlon)
    return split_table(np.stack([zero, two], 0)), split_table(ones)


def latitude_table(nlat):
    rows = np.sin(np.pi * (np.arange(nlat) + 0.5) / nlat)
    faces = np.sin(np.pi * np.arange(nlat + 1) / nlat)
    faces[0] = faces[-1] = 0.0
    table = np.concatenate([faces / 24.0, rows, 1.0 / rows]).astype(np.float32)
    return table, float(np.sum(rows))


def shifted(x, s):
    return jnp.concatenate([x[:, s:], x[:, :s]], axis=1)


def halves(x):
    high = x.astype(BF)
    return high, (x - high.astype(F32)).astype(BF)


def product(x, high_table, low_table):
    high, low = halves(x)
    rows = x.shape[0]
    both = jnp.dot(
        jnp.concatenate([high, low], axis=0), high_table, preferred_element_type=F32
    )
    return both[:rows] + both[rows:] + jnp.dot(high, low_table, preferred_element_type=F32)


def kernel(
    n, area,
    lat_hbm, flags_hbm, cutoffs_hbm, rates_hbm, thresholds_hbm,
    h_hbm, z_hbm, m_hbm, quarter_hbm, half_hbm,
    out,
    lat_ref, flags_ref, cutoffs_ref, rates_ref, thresholds_ref,
    h, z, m, quarter_t, half_t, base, sides, part, mine, others,
    hl, ml, hr, mr,
    in_sem, halo_send, halo_recv, sum_send, sum_recv,
):
    rows, levels, nlon = h.shape
    me = lax.axis_index("lat")
    first = me * rows
    groups = levels // GROUP
    width = levels // CHUNKS

    loads = [
        pltpu.make_async_copy(src, dst, in_sem.at[i])
        for i, (src, dst) in enumerate(
            [
                (h_hbm, h), (z_hbm, z), (m_hbm, m), (quarter_hbm, quarter_t), (half_hbm, half_t),
                (lat_hbm, lat_ref), (flags_hbm, flags_ref), (cutoffs_hbm, cutoffs_ref),
                (rates_hbm, rates_ref), (thresholds_hbm, thresholds_ref),
            ]
        )
    ]
    for i in (0, 2, 1, 5, 6, 7, 8, 9):
        loads[i].start()
    nlat = rows * n

    def face_scale(f):
        return lat_ref[first + f]

    def row_weight(r):
        return lat_ref[nlat + 1 + first + r]

    def row_scale(r):
        return lat_ref[2 * nlat + 1 + first + r]

    barrier = pltpu.get_barrier_semaphore()

    def greet(o, c):
        pl.semaphore_signal(barrier, inc=1, device_id={"lat": lax.rem(me + o, n)})
        return c

    lax.fori_loop(1, n, greet, 0)
    pl.semaphore_wait(barrier, n - 1)

    def halo_copies(c, side):
        at = pl.ds(c * width, width)
        if side == 0:
            pairs = [
                (h.at[pl.ds(rows - 2, 2), at], hl.at[:, at]),
                (m.at[rows - 1, at], ml.at[at]),
            ]
            target = me + 1
        else:
            pairs = [
                (h.at[pl.ds(0, 2), at], hr.at[:, at]),
                (m.at[0, at], mr.at[at]),
            ]
            target = me - 1
        return [
            pltpu.make_async_remote_copy(
                src, dst, halo_send.at[side, c, i], halo_recv.at[side, c, i],
                device_id={"lat": target},
            )
            for i, (src, dst) in enumerate(pairs)
        ]

    def each(side, chunks, act):
        @pl.when(me < n - 1 if side == 0 else me > 0)
        def _():
            for c in chunks:
                for copy in halo_copies(c, side):
                    act(copy)

    def start_halo(chunks):
        each(0, chunks, lambda copy: copy.start())
        each(1, chunks, lambda copy: copy.start())

    loads[0].wait()
    loads[2].wait()
    start_halo(range(IN_FLIGHT))
    loads[3].start()
    loads[4].start()

    @pl.when(me == 0)
    def _():
        hl[...] = jnp.zeros_like(hl)
        ml[...] = jnp.zeros_like(ml)

    @pl.when(me == n - 1)
    def _():
        hr[...] = jnp.zeros_like(hr)
        mr[...] = jnp.zeros_like(mr)

    lane = lax.broadcasted_iota(jnp.int32, (levels, levels), 1)
    diagonal = lane == lax.broadcasted_iota(jnp.int32, (levels, levels), 0)

    def column(row):
        spread = jnp.where(diagonal, jnp.broadcast_to(row, (levels, levels)), 0.0)
        return jnp.sum(spread, axis=1, keepdims=True)

    for i in (5, 6, 7, 8, 9):
        loads[i].wait()
    sides[0] = jnp.broadcast_to(column(rates_ref[...]), (levels, 128))
    sides[1] = jnp.broadcast_to(column(thresholds_ref[...]), (levels, 128))

    loads[1].wait()

    def local_terms(g, carry):
        at = pl.ds(pl.multiple_of(g * GROUP, GROUP), GROUP)
        rate = sides[0, at, :][:, :1]
        threshold = sides[1, at, :][:, :1]
        weighted = jnp.zeros((GROUP, nlon), F32)
        for r in range(rows):
            hh = h[r, at, :]
            zz = z[r, at, :]
            face = 7.0 * (hh + shifted(hh, 1)) - (shifted(hh, nlon - 1) + shifted(hh, 2))
            flux = (zz + shifted(zz, 1)) * face * (1.0 / 24.0)
            source = -rate * jnp.log(1.0 + jnp.exp(hh - threshold))
            base[r, at, :] = hh - (flux - shifted(flux, nlon - 1)) + source
            weighted = weighted + source * row_weight(r)
        total = jnp.sum(weighted, axis=1, keepdims=True)
        part[at, :] = jnp.broadcast_to(total, (GROUP, 128))
        return carry

    lax.fori_loop(0, groups, local_terms, 0)

    wide = lax.broadcasted_iota(jnp.int32, (levels, 128), 1)
    tall = lax.broadcasted_iota(jnp.int32, (levels, 128), 0)
    mine[...] = jnp.sum(jnp.where(wide == tall, part[...], 0.0), axis=0, keepdims=True)

    def sum_copy(o):
        return pltpu.make_async_remote_copy(
            mine, others.at[o - 1], sum_send.at[o - 1], sum_recv.at[o - 1],
            device_id={"lat": lax.rem(me + o, n)},
        )

    def send_sum(o, c):
        sum_copy(o).start()
        return c

    lax.fori_loop(1, n, send_sum, 0)

    quarter, half = nlon // 4, nlon // 2

    def factors(length, step, offset):
        k = lax.broadcasted_iota(jnp.int32, (1, length), 1) * step + offset
        k = jnp.maximum(jnp.minimum(k, nlon - k), 1).astype(F32)
        out = []
        for r in range(rows):
            ratio = cutoffs_ref[first + r].astype(F32) / k
            factor = (1.0 - jnp.minimum(1.0, ratio * ratio)) * (1.0 / nlon)
            on = jnp.where(flags_ref[first + r] > 0, 1.0, 0.0)
            out.append(factor * on)
        return out

    all_factors = [factors(quarter, 4, 0), factors(quarter, 4, 2), factors(half, 2, 1)]

    def removed(x, high_table, low_table, factor):
        spectrum = product(x, high_table, low_table).reshape(rows, -1, x.shape[1])
        scaled = jnp.concatenate([spectrum[r] * factor[r] for r in range(rows)], axis=0)
        return product(scaled, high_table, low_table)

    polar = jnp.logical_or(first < nlat // 4, first + rows > nlat - nlat // 4)

    def merid(c):
        def body(g, carry):
            at = pl.ds(pl.multiple_of(c * width + g * GROUP, GROUP), GROUP)

            def height(i):
                return hl[i + 2, at, :] if i < 0 else hr[i - rows, at, :] if i >= rows else h[i, at, :]

            def speed(i):
                return ml[at, :] if i < 0 else mr[at, :] if i >= rows else m[i, at, :]

            previous = None
            for f in range(rows + 1):
                face = 7.0 * (height(f - 1) + height(f)) - (height(f - 2) + height(f + 1))
                flux = (speed(f - 1) + speed(f)) * face * face_scale(f)
                if f > 0:
                    base[f - 1, at, :] -= (flux - previous) * row_scale(f - 1)
                previous = flux
            return carry

        lax.fori_loop(0, width // GROUP, body, 0)

    def receive(c):
        @pl.when(me > 0)
        def _():
            for copy in halo_copies(c, 0):
                copy.wait_recv()

        @pl.when(me < n - 1)
        def _():
            for copy in halo_copies(c, 1):
                copy.wait_recv()

        each(0, [c], lambda copy: copy.wait_send())
        each(1, [c], lambda copy: copy.wait_send())
        if c + IN_FLIGHT < CHUNKS:
            start_halo([c + IN_FLIGHT])

    mean = None
    for low, high in FILTERED:
        for c in range(low, high):
            receive(c)
            merid(c)
        if low == 0:
            loads[3].wait()
            loads[4].wait()
            def wait_sum(o, carry):
                sum_copy(o).wait()
                return carry

            lax.fori_loop(1, n, wait_sum, 0)
            total = mine[...] + jnp.sum(others[...], axis=0)
            mean = column(total[:, :levels]) * (1.0 / area)
        at = pl.ds(low * width, (high - low) * width)
        level_mean = mean[low * width : high * width][None]

        @pl.when(polar)
        def _():
            x = base[:, at, :].reshape(rows * (high - low) * width, nlon)
            near, far = x[:, :half], x[:, half:]
            even, odd = near + far, near - far
            left, right = even[:, :quarter], even[:, quarter:]
            zero = removed(left + right, quarter_t[0, 0], quarter_t[1, 0], all_factors[0])
            two = removed(left - right, quarter_t[0, 1], quarter_t[1, 1], all_factors[1])
            ones = removed(odd, half_t[0], half_t[1], all_factors[2])
            even = jnp.concatenate([zero + two, zero - two], axis=1)
            kept = jnp.concatenate([near - even - ones, far - even + ones], axis=1)
            out[:, at, :] = kept.reshape(rows, (high - low) * width, nlon) - level_mean

        @pl.when(jnp.logical_not(polar))
        def _():
            out[:, at, :] = base[:, at, :] - level_mean


def local(n, height, zonal_courant, merid_courant, rates, thresholds, flags, cutoffs):
    rows, levels, nlon = height.shape
    table, row_sum = latitude_table(rows * n)
    quarter_t, half_t = filter_tables(nlon)
    hbm = pl.BlockSpec(memory_space=pltpu.HBM)
    vmem = pl.BlockSpec(memory_space=pltpu.VMEM)
    block = pltpu.VMEM(height.shape, F32)
    return pl.pallas_call(
        functools.partial(kernel, n, nlon * row_sum),
        out_shape=pltpu.VMEM(height.shape, F32),
        in_specs=[hbm] * 10,
        out_specs=vmem,
        scratch_shapes=[
            pltpu.SMEM(table.shape, F32),
            pltpu.SMEM(flags.shape, jnp.int32),
            pltpu.SMEM(cutoffs.shape, jnp.int32),
            pltpu.VMEM((1, levels), F32),
            pltpu.VMEM((1, levels), F32),
            block, block, block,
            pltpu.VMEM(quarter_t.shape, BF),
            pltpu.VMEM(half_t.shape, BF),
            block,
            pltpu.VMEM((2, levels, 128), F32),
            pltpu.VMEM((levels, 128), F32),
            pltpu.VMEM((1, 128), F32),
            pltpu.VMEM((n - 1, 1, 128), F32),
            pltpu.VMEM((2, levels, nlon), F32),
            pltpu.VMEM((levels, nlon), F32),
            pltpu.VMEM((2, levels, nlon), F32),
            pltpu.VMEM((levels, nlon), F32),
            pltpu.SemaphoreType.DMA((10,)),
            pltpu.SemaphoreType.DMA((2, CHUNKS, 2)),
            pltpu.SemaphoreType.DMA((2, CHUNKS, 2)),
            pltpu.SemaphoreType.DMA((n - 1,)),
            pltpu.SemaphoreType.DMA((n - 1,)),
        ],
        compiler_params=pltpu.CompilerParams(
            collective_id=0, has_side_effects=True, vmem_limit_bytes=62 * 1024 * 1024
        ),
    )(
        jnp.asarray(table), flags, cutoffs, rates[None, :], thresholds[None, :],
        height, zonal_courant, merid_courant, jnp.asarray(quarter_t), jnp.asarray(half_t),
    )


def solution(mesh):
    return jax.shard_map(
        functools.partial(local, mesh.shape["lat"]),
        mesh=mesh,
        in_specs=(
            P(("member", "lat"), None, None),
            P(("member", "lat"), None, None),
            P(("member", "lat"), None, None),
            P("member"),
            P("member"),
            P(),
            P(),
        ),
        out_specs=P(("member", "lat"), None, None),
        check_vma=False,
    )
```
